256 devices in a mesh: grp: 4 (over y, x), wide: 64 (over z, core).
Axes of the slice: x: 2, y: 2, z: 32, core: 2. Of those that a mesh axis runs over, the one named last changes fastest.
The devices are a block of a 4x8x32 slice.
Arguments:
- kv_prefill: bfloat16 [2, 32, 8, 8192, 128], P(None, 'grp', None, 'wide'), parts along dimension 1, may hold values from -4 to 4
- queries: bfloat16 [256, 1024], P(('grp', 'wide')), parts along dimension 0, may hold values from -512 to 512
- fresh_kv: bfloat16 [2, 256, 128], P(None, ('grp', 'wide')), parts along dimension 1, may hold values from -4 to 4
- lengths: int32 [32], P('grp'), parts along dimension 0, may hold values from 1 to 8191, as said below
- decode_slot_pair: int32 [256], P('grp'), parts along dimension 0, may hold values from 0 to 63, each once
Outputs:
- decode_cache: bfloat16 [2, 256, 8192, 128], P(None, ('grp', 'wide')), parts along dimension 1
- attention: bfloat16 [256, 1024], P(('grp', 'wide')), parts along dimension 0
The draws below stay inside these ranges and needn't reach their ends.
There are 4 independent parts, one for each index of `grp`. The reference program is written for one: setup_inputs(seed, part) draws one part's arguments, and reference() takes and returns one part's arrays. A program takes and returns all parts, laid end to end along the dimension named above; each array names one. Nothing has to cross between parts.
Inputs may be any that keep to these rules, and one draw needn't show every extreme that they name: `lengths`: every draw holds a sequence of length 8191 and one of length 1. `decode_slot_pair`: slot j lies on the device of wide with index j // (64 / 64).
All inputs are finite; a program needn't handle non-finite values.
Results may differ from the reference program's by a relative error of at most 0.001.
Values may be sent and summed in bfloat16 or wider, within the bound.
A program may use at most 64 MiB of HBM per device.

```python
import math
import jax
import jax.numpy as jnp
from jax import lax

QUERY_HEADS = 64
KEY_VALUE_HEADS = 8
HEAD_SIZE = 128
GROUP_SEQUENCES = 8
CACHE_LENGTH = 8192
PAIR_COUNT = 64


def common_sample(key):
    every_key_row = jnp.clip(jax.random.normal(jax.random.fold_in(key, 11), (2, GROUP_SEQUENCES, KEY_VALUE_HEADS, CACHE_LENGTH, HEAD_SIZE), jnp.float32), -4.0, 4.0)
    every_query_row = jnp.clip(jax.random.normal(jax.random.fold_in(key, 12), (PAIR_COUNT, QUERY_HEADS // KEY_VALUE_HEADS, HEAD_SIZE), jnp.float32), -4.0, 4.0)
    fresh_all = jnp.clip(jax.random.normal(jax.random.fold_in(key, 13), (2, PAIR_COUNT, HEAD_SIZE), jnp.float32), -4.0, 4.0)
    return (every_key_row, every_query_row, fresh_all)


def draw_kv_prefill(key, part):
    return common_sample(key)[0].astype(jnp.bfloat16)


def draw_queries(key, part):
    return common_sample(key)[1].reshape(PAIR_COUNT, QUERY_HEADS // KEY_VALUE_HEADS * HEAD_SIZE).astype(jnp.bfloat16)


def draw_fresh_kv(key, part):
    return common_sample(key)[2].astype(jnp.bfloat16)


def draw_lengths(key, part):
    values = jax.random.randint(jax.random.fold_in(key, 21), (GROUP_SEQUENCES,), 1, CACHE_LENGTH, dtype=jnp.int32)
    order = jax.random.permutation(jax.random.fold_in(key, 22), GROUP_SEQUENCES)
    values = values.at[order[0]].set(CACHE_LENGTH - 1)
    values = values.at[order[1]].set(1)
    return values


def setup_inputs(seed: int = 0, part: int = 0) -> dict:
    splits = jax.random.split(jax.random.key(seed), 6)
    own_keys = jax.random.split(jax.random.fold_in(splits[5], part), 6)
    return {
        "kv_prefill": draw_kv_prefill(jax.random.fold_in(jax.random.fold_in(splits[5], part), 71), part),
        "queries": draw_queries(jax.random.fold_in(jax.random.fold_in(splits[5], part), 71), part),
        "fresh_kv": draw_fresh_kv(jax.random.fold_in(jax.random.fold_in(splits[5], part), 71), part),
        "lengths": draw_lengths(jax.random.fold_in(jax.random.fold_in(splits[5], part), 71), part),
        "decode_slot_pair": jax.random.permutation(own_keys[4], PAIR_COUNT).astype(jnp.int32),
    }


NEG_FILL = -1e+30

def reference(kv_prefill, queries, fresh_kv, lengths, decode_slot_pair):
    kv_items = kv_prefill.reshape(2, PAIR_COUNT, CACHE_LENGTH, HEAD_SIZE)
    positions = jnp.arange(CACHE_LENGTH, dtype=jnp.int32)
    pair_length = jnp.repeat(lengths, KEY_VALUE_HEADS)
    in_prompt = positions[None, :] < pair_length[:, None]
    cache_all = jnp.where(in_prompt[None, :, :, None], kv_items, jnp.zeros((), kv_items.dtype))
    at_new = positions[None, :] == pair_length[:, None]
    cache_all = jnp.where(at_new[None, :, :, None], fresh_kv[:, :, None, :], cache_all)
    decode_cache = jnp.take(cache_all, decode_slot_pair, axis=1)
    slot_len = jnp.take(pair_length, decode_slot_pair)
    decode_slot_query = jnp.take(queries, decode_slot_pair, axis=0).reshape(PAIR_COUNT, QUERY_HEADS // KEY_VALUE_HEADS, HEAD_SIZE)
    softmax_scale = 1.0 / math.sqrt(HEAD_SIZE)

    def attend_one(packed):
        query_rows, item_cache, limit = packed
        scores = jnp.dot(query_rows, item_cache[0].T, preferred_element_type=jnp.float32) * softmax_scale
        visible = positions <= limit
        scores = jnp.where(visible[None, :], scores, NEG_FILL)
        top_score = lax.optimization_barrier(jnp.max(scores, axis=1, keepdims=True))
        weights = jnp.where(visible[None, :], jnp.exp(scores - top_score), 0.0)
        total = lax.optimization_barrier(jnp.sum(weights, axis=1, keepdims=True))
        summed = jnp.dot(weights, item_cache[1].astype(jnp.float32), precision=lax.Precision.HIGHEST)
        return (summed / total).reshape(-1).astype(jnp.bfloat16)
    attention = lax.map(attend_one, (decode_slot_query, jnp.moveaxis(decode_cache, 1, 0), slot_len))
    return (decode_cache, attention)
```

```python
import functools
import math

import jax
import jax.numpy as jnp
from jax import lax
from jax.experimental import pallas as pl
from jax.experimental.pallas import tpu as pltpu
from jax.sharding import PartitionSpec as P

MESH = pl.DeviceIdType.MESH
NEG_FILL = -1e30
ROW_TILE = 16
CHUNK = 1024


def exchange_kernel(
    devices,
    perm_ref,
    query_ref,
    fresh_ref,
    kv_ref,
    gathered_ref,
    own_ref,
    stage,
    ordered,
    rows,
    stage_sem,
    local_sem,
    send_sem,
    recv_sem,
    row_send,
    row_recv,
    near_sem,
):
    chips = devices // 2
    half = chips // 2
    me = lax.axis_index("wide")
    chip = me // 2
    core = lax.rem(me, 2)
    partner = chip * 2 + 1 - core
    local_len = kv_ref.shape[2]

    def device(offset, which):
        return lax.rem(chip + offset + chips, chips) * 2 + which

    def remote(src, dst, send, recv, target):
        return pltpu.make_async_remote_copy(
            src_ref=src,
            dst_ref=dst,
            send_sem=send,
            recv_sem=recv,
            device_id={"wide": target},
            device_id_type=MESH,
        )

    def signal(sem, target):
        pl.semaphore_signal(sem, inc=1, device_id={"wide": target}, device_id_type=MESH)

    barrier = pltpu.get_barrier_semaphore()
    signal(barrier, partner)
    for offset in (1, -1):
        for which in (0, 1):
            signal(barrier, device(offset, which))
    fill = pltpu.make_async_copy(kv_ref, stage, stage_sem)
    fill.start()
    query = query_ref[...].astype(jnp.float32)
    head_dim = kv_ref.shape[3]
    group_size = query.shape[1] // head_dim
    parts = [query[:, g * head_dim : (g + 1) * head_dim] for g in range(group_size)]
    parts.append(fresh_ref[...].astype(jnp.float32))
    parts.append(jnp.zeros((ROW_TILE - group_size - 2, head_dim), jnp.float32))
    rows[0, 0] = jnp.concatenate(parts, axis=0).astype(jnp.bfloat16)
    fill.wait()

    def place(slot, carry):
        ordered[slot] = stage[:, perm_ref[slot]]
        return carry

    lax.fori_loop(0, devices, place, 0)
    pl.semaphore_wait(barrier, 5)

    final = gathered_ref.at[:, pl.ds(me * local_len, local_len)]
    keep = pltpu.make_async_copy(ordered.at[me], final, local_sem)
    keep.start()

    def send_block(target):
        remote(ordered.at[target], final, send_sem, recv_sem, target).start()

    def send_both(distance, cores=(0, 1)):
        for which in cores:
            for sign in (1, -1):
                send_block(device(sign * distance, which))

    def widen(level):
        reach = 1 << level
        for sign in (1, -1):
            signal(near_sem.at[level], device(sign * reach, core))
        pl.semaphore_wait(near_sem.at[level], 2)

    send_block(partner)
    send_both(1, (0,))
    sent_to = 1
    level = 0
    while (1 << level) < half:
        widen(level)
        level += 1
        if level < half.bit_length() - 1:
            for distance in range(sent_to + 1, min((1 << level), 5) + 1):
                send_both(distance)
                sent_to = distance

    turn = 1 - 2 * core

    def row_copy(step):
        size = 1 << step
        return remote(
            rows.at[0, pl.ds(0, size)],
            rows.at[0, pl.ds(size, size)],
            row_send.at[step],
            row_recv.at[step],
            device(turn * (chips >> (step + 1)), core),
        )

    send_block(device(half, 0))
    send_block(device(half, 1))
    row_steps = chips.bit_length() - 1
    row_copy(0).start()
    step = 0
    distances = list(range(half - 1, sent_to, -1))
    for number, distance in enumerate(distances):
        send_both(distance)
        if number % 2 == 1:
            if step < row_steps:
                row_copy(step).wait()
                step += 1
                if step < row_steps:
                    row_copy(step).start()
    send_both(1, (1,))
    while step < row_steps:
        row_copy(step).wait()
        step += 1
        if step < row_steps:
            row_copy(step).start()
    across = remote(rows.at[0], rows.at[1], row_send.at[row_steps], row_recv.at[row_steps], partner)
    across.start()
    across.wait()

    item = perm_ref[me]
    item_core = lax.rem(item, 2)
    same = 1 - lax.rem(item_core + core, 2)
    offset = lax.rem((1 - 2 * item_core) * (chip - item // 2) + chips, chips)
    place_of = 0
    for bit in range(row_steps):
        place_of += lax.rem(offset // (1 << bit), 2) * (chips >> (bit + 1))
    own_ref[...] = rows[1 - same, place_of]

    keep.wait()
    many = ordered.at[pl.ds(0, devices - 1)]
    everything = remote(many, many, send_sem, recv_sem, partner)
    everything.wait_send()
    everything.wait_recv()


def exchange(perm, queries, fresh, kv, devices):
    items, local_len, head_dim = kv.shape[1:]
    chips = devices // 2
    row_steps = chips.bit_length() - 1
    any_space = pl.BlockSpec(memory_space=pl.ANY)
    vmem = pl.BlockSpec(memory_space=pltpu.VMEM)
    block = (2, local_len, head_dim)
    return pl.pallas_call(
        functools.partial(exchange_kernel, devices),
        out_shape=(
            jax.ShapeDtypeStruct((2, devices * local_len, head_dim), kv.dtype),
            jax.ShapeDtypeStruct((ROW_TILE, head_dim), kv.dtype),
        ),
        in_specs=[pl.BlockSpec(memory_space=pltpu.SMEM), vmem, vmem, any_space],
        out_specs=(any_space, vmem),
        scratch_shapes=[
            pltpu.VMEM((2, items, local_len, head_dim), kv.dtype),
            pltpu.VMEM((items, *block), kv.dtype),
            pltpu.VMEM((2, chips, ROW_TILE, head_dim), kv.dtype),
            pltpu.SemaphoreType.DMA,
            pltpu.SemaphoreType.DMA,
            pltpu.SemaphoreType.DMA,
            pltpu.SemaphoreType.DMA,
            pltpu.SemaphoreType.DMA((row_steps + 1,)),
            pltpu.SemaphoreType.DMA((row_steps + 1,)),
            pltpu.SemaphoreType.REGULAR((row_steps,)),
        ],
        compiler_params=pltpu.CompilerParams(collective_id=0, has_side_effects=True),
        name="exchange",
    )(perm, queries, fresh, kv)


def attend_kernel(
    head_count, perm_ref, length_ref, own_ref, gathered_ref, cache_ref, out_ref,
    tiles, zeros, scores, in_sems, out_sem,
):
    me = lax.axis_index("wide")
    length = length_ref[perm_ref[me] // head_count]
    total_len, head_dim = tiles.shape[1:]
    group_size = scores.shape[0]
    chunk = zeros.shape[0]
    chunk_count = total_len // chunk
    live = length // chunk + 1
    last = live - 1

    def part(ref, kind, c):
        return ref.at[kind, pl.ds(pl.multiple_of(c * chunk, chunk), chunk)]

    def fetch(kind, c):
        return pltpu.make_async_copy(part(gathered_ref, kind, c), part(tiles, kind, c), in_sems.at[kind, c])

    def store(kind, c):
        return pltpu.make_async_copy(part(tiles, kind, c), part(cache_ref, kind, c), out_sem)

    def blank(kind, c):
        return pltpu.make_async_copy(zeros, part(cache_ref, kind, c), out_sem)

    for kind in (0, 1):
        lax.fori_loop(0, live, lambda c, x, kind=kind: (fetch(kind, c).start(), x)[1], 0)
    zeros[...] = jnp.zeros_like(zeros)

    def settle(kind):
        start = pl.multiple_of(last * chunk, chunk)
        tile = tiles[kind, pl.ds(start, chunk)].astype(jnp.float32)
        position = start + lax.broadcasted_iota(jnp.int32, tile.shape, 0)
        fresh = own_ref[pl.ds(group_size, 2)].astype(jnp.float32)[kind : kind + 1]
        tile = jnp.where(position < length, tile, jnp.where(position == length, fresh, 0.0))
        tiles[kind, pl.ds(start, chunk)] = tile.astype(tiles.dtype)

    query = own_ref[...][:group_size]
    scale = 1.0 / math.sqrt(head_dim)

    def score(c, top):
        fetch(0, c).wait()

        @pl.when(c == last)
        def _():
            settle(0)

        start = pl.multiple_of(c * chunk, chunk)
        s = lax.dot_general(
            query, tiles[0, pl.ds(start, chunk)], (((1,), (1,)), ((), ())),
            preferred_element_type=jnp.float32,
        ) * scale
        position = start + lax.broadcasted_iota(jnp.int32, s.shape, 1)
        s = jnp.where(position <= length, s, NEG_FILL)
        scores[:, pl.ds(start, chunk)] = s
        store(0, c).start()
        return jnp.maximum(top, jnp.max(s, axis=1, keepdims=True))

    top = lax.fori_loop(0, live, score, jnp.full((group_size, 1), NEG_FILL, jnp.float32))

    def gather(c, carry):
        total, summed = carry
        fetch(1, c).wait()

        @pl.when(c == last)
        def _():
            settle(1)

        start = pl.multiple_of(c * chunk, chunk)
        s = scores[:, pl.ds(start, chunk)]
        position = start + lax.broadcasted_iota(jnp.int32, s.shape, 1)
        weight = jnp.where(position <= length, jnp.exp(s - top), 0.0)
        high = weight.astype(jnp.bfloat16)
        low = (weight - high.astype(jnp.float32)).astype(jnp.bfloat16)
        both = jnp.concatenate([high, low], axis=0)
        summed = summed + jnp.dot(both, tiles[1, pl.ds(start, chunk)], preferred_element_type=jnp.float32)
        store(1, c).start()
        return total + jnp.sum(weight, axis=1, keepdims=True), summed

    for kind in (0, 1):
        lax.fori_loop(live, chunk_count, lambda c, x, kind=kind: (blank(kind, c).start(), x)[1], 0)

    total, summed = lax.fori_loop(
        0, live, gather,
        (jnp.zeros((group_size, 1), jnp.float32), jnp.zeros((2 * group_size, head_dim), jnp.float32)),
    )
    result = (summed[:group_size] + summed[group_size:]) / total
    for g in range(group_size):
        out_ref[:, g * head_dim : (g + 1) * head_dim] = result[g : g + 1].astype(out_ref.dtype)
    pltpu.make_async_copy(tiles, cache_ref, out_sem).wait()


def attend(perm, lengths, own, gathered, head_count, group_size):
    kinds, total_len, head_dim = gathered.shape
    chunk = min(CHUNK, total_len)
    vmem = pl.BlockSpec(memory_space=pltpu.VMEM)
    smem = pl.BlockSpec(memory_space=pltpu.SMEM)
    any_space = pl.BlockSpec(memory_space=pl.ANY)
    return pl.pallas_call(
        functools.partial(attend_kernel, head_count),
        out_shape=(
            jax.ShapeDtypeStruct(gathered.shape, gathered.dtype),
            jax.ShapeDtypeStruct((1, group_size * head_dim), gathered.dtype),
        ),
        in_specs=[smem, smem, vmem, any_space],
        out_specs=(any_space, vmem),
        scratch_shapes=[
            pltpu.VMEM(gathered.shape, gathered.dtype),
            pltpu.VMEM((chunk, head_dim), gathered.dtype),
            pltpu.VMEM((group_size, total_len), jnp.float32),
            pltpu.SemaphoreType.DMA((kinds, total_len // chunk)),
            pltpu.SemaphoreType.DMA,
        ],
        name="attend",
    )(perm, lengths, own, gathered)


def local(kv_prefill, queries, fresh_kv, lengths, decode_slot_pair):
    devices = lax.axis_size("wide")
    kinds, seq_count, head_count, local_len, head_dim = kv_prefill.shape
    kv_rows = kv_prefill.reshape(kinds, seq_count * head_count, local_len, head_dim)
    fresh = fresh_kv.reshape(kinds, head_dim)
    gathered, own = exchange(decode_slot_pair, queries, fresh, kv_rows, devices)
    cache, attention = attend(
        decode_slot_pair, lengths, own, gathered, head_count, queries.shape[1] // head_dim
    )
    return cache[:, None], attention


def solution(mesh):
    in_specs = (
        P(None, "grp", None, "wide", None),
        P(("grp", "wide"), None),
        P(None, ("grp", "wide"), None),
        P("grp"),
        P("grp"),
    )
    out_specs = (P(None, ("grp", "wide"), None, None), P(("grp", "wide"), None))
    return jax.shard_map(local, mesh=mesh, in_specs=in_specs, out_specs=out_specs, check_vma=False)
```

```python
import functools
import math

import jax
import jax.numpy as jnp
from jax import lax
from jax.experimental import pallas as pl
from jax.experimental.pallas import tpu as pltpu
from jax.sharding import PartitionSpec as P

MESH = pl.DeviceIdType.MESH
NEG_FILL = -1e30
PAIR = 2
CHUNK = 1024
EARLY = 8
EXCHANGE_VMEM = 58 << 20
ATTEND_VMEM = 12 << 20


def exchange_kernel(
    devices,
    perm_ref,
    query_ref,
    fresh_ref,
    kv_ref,
    gathered_ref,
    own_ref,
    stage,
    ordered,
    rows,
    passing,
    stage_sem,
    local_sem,
    send_sem,
    recv_sem,
    row_send,
    row_recv,
    near_sem,
    pass_send,
    pass_recv,
):
    chips = devices // 2
    half = chips // 2
    me = lax.axis_index("wide")
    chip = me // 2
    core = lax.rem(me, 2)
    partner = chip * 2 + 1 - core
    local_len = kv_ref.shape[2]

    def device(offset, which):
        return lax.rem(chip + offset + chips, chips) * 2 + which

    def remote(src, dst, send, recv, target):
        return pltpu.make_async_remote_copy(
            src_ref=src,
            dst_ref=dst,
            send_sem=send,
            recv_sem=recv,
            device_id={"wide": target},
            device_id_type=MESH,
        )

    def signal(sem, target):
        pl.semaphore_signal(sem, inc=1, device_id={"wide": target}, device_id_type=MESH)

    barrier = pltpu.get_barrier_semaphore()
    signal(barrier, partner)
    for offset in (1, -1):
        for which in (0, 1):
            signal(barrier, device(offset, which))
    fill = pltpu.make_async_copy(kv_ref, stage, stage_sem)
    fill.start()
    head_dim = kv_ref.shape[3]
    group_size = query_ref.shape[1] // head_dim
    query = query_ref[...].astype(jnp.float32)
    for g in range(0, group_size, PAIR):
        heads = [query[:, h * head_dim : (h + 1) * head_dim] for h in range(g, g + PAIR)]
        rows[0, 0, g // PAIR] = jnp.concatenate(heads, axis=0).astype(jnp.bfloat16)
    rows[0, 0, group_size // PAIR] = fresh_ref[...]
    fill.wait()

    def place(slot):
        ordered[slot] = stage[:, perm_ref[slot]]

    def place_span(first, last):
        def one(k, carry):
            place(lax.rem(chip * 2 + (devices + first) + k, devices))
            return carry

        lax.fori_loop(0, last - first, one, 0)

    place_span(-4, 6)
    pl.semaphore_wait(barrier, 5)

    final = gathered_ref.at[:, pl.ds(me * local_len, local_len)]
    keep = pltpu.make_async_copy(ordered.at[me], final, local_sem)
    keep.start()

    def send_block(target):
        remote(ordered.at[target], final, send_sem, recv_sem, target).start()

    def send_both(distance, cores=(0, 1)):
        for which in cores:
            for sign in (1, -1):
                send_block(device(sign * distance, which))

    def widen(level):
        reach = 1 << level
        for sign in (1, -1):
            signal(near_sem.at[level], device(sign * reach, core))
        pl.semaphore_wait(near_sem.at[level], 2)

    send_block(partner)
    send_both(1, (1,))
    place_span(6, devices - 4)
    sent_to = 1
    level = 0
    while (1 << level) < half:
        widen(level)
        level += 1
        if level < half.bit_length() - 1:
            for distance in range(sent_to + 1, min((1 << level), EARLY) + 1):
                send_both(distance, (distance % 2,))
                sent_to = distance

    turn = 1 - 2 * core

    def row_copy(step):
        size = 1 << step
        return remote(
            rows.at[0, pl.ds(0, size)],
            rows.at[0, pl.ds(size, size)],
            row_send.at[step],
            row_recv.at[step],
            device(turn * (chips >> (step + 1)), core),
        )

    side = jnp.where(chip >= half, 1, -1)

    def turns(c):
        quarter = chips // 4
        return ((c >= chips - quarter) & (lax.rem(c, 2) == 0)) | ((c < quarter) & (lax.rem(c, 2) == 1))

    turned = turns(chip)
    relaying = turns(lax.rem(chip + side + chips, chips))

    def detour():
        both = ordered.at[pl.ds(device(half, 0), 2)]
        return remote(both, passing, pass_send.at[0], pass_recv, device(-side, core))

    def forward(which):
        origin = device(side, core)
        return remote(
            passing.at[which],
            gathered_ref.at[:, pl.ds(origin * local_len, local_len)],
            pass_send.at[1 + which],
            recv_sem,
            device(half + side, which),
        )

    @pl.when(turned)
    def _():
        detour().start()

    @pl.when(jnp.logical_not(turned))
    def _():
        send_block(device(half, 0))
        send_block(device(half, 1))

    row_steps = chips.bit_length() - 1
    row_copy(0).start()
    step = 0
    rounds = [(distance, (0, 1)) for distance in range(half - 1, sent_to, -1)]
    rounds += [(distance, (1 - distance % 2,)) for distance in range(sent_to, 0, -1)]
    for number, (distance, cores) in enumerate(rounds):
        send_both(distance, cores)
        if number == 2:

            @pl.when(relaying)
            def _():
                detour().wait_recv()
                forward(0).start()
                forward(1).start()

        if number % 2 == 1:
            if step < row_steps:
                row_copy(step).wait()
                step += 1
                if step < row_steps:
                    row_copy(step).start()
    while step < row_steps:
        row_copy(step).wait()
        step += 1
        if step < row_steps:
            row_copy(step).start()
    across = remote(rows.at[0], rows.at[1], row_send.at[row_steps], row_recv.at[row_steps], partner)
    across.start()
    across.wait()

    item = perm_ref[me]
    item_core = lax.rem(item, 2)
    same = 1 - lax.rem(item_core + core, 2)
    offset = lax.rem((1 - 2 * item_core) * (chip - item // 2) + chips, chips)
    place_of = 0
    for bit in range(row_steps):
        place_of += lax.rem(offset // (1 << bit), 2) * (chips >> (bit + 1))
    own_ref[...] = rows[1 - same, place_of]

    keep.wait()
    def blocks(count):
        many = ordered.at[pl.ds(0, count)]
        return remote(many, many, send_sem, recv_sem, partner)

    @pl.when(turned)
    def _():
        detour().wait_send()
        blocks(devices - 3).wait_send()

    @pl.when(jnp.logical_not(turned))
    def _():
        blocks(devices - 1).wait_send()

    @pl.when(relaying)
    def _():
        forward(0).wait_send()
        forward(1).wait_send()

    blocks(devices - 1).wait_recv()


def exchange(perm, queries, fresh, kv, devices):
    items, local_len, head_dim = kv.shape[1:]
    chips = devices // 2
    row_steps = chips.bit_length() - 1
    any_space = pl.BlockSpec(memory_space=pl.ANY)
    vmem = pl.BlockSpec(memory_space=pltpu.VMEM)
    row = (queries.shape[1] // head_dim // PAIR + 1, PAIR, head_dim)
    return pl.pallas_call(
        functools.partial(exchange_kernel, devices),
        out_shape=(
            pltpu.VMEM((2, devices * local_len, head_dim), kv.dtype),
            pltpu.VMEM(row, kv.dtype),
        ),
        in_specs=[pl.BlockSpec(memory_space=pltpu.SMEM), vmem, vmem, any_space],
        out_specs=(vmem, vmem),
        scratch_shapes=[
            pltpu.VMEM((2, items, local_len, head_dim), kv.dtype),
            pltpu.VMEM((items, 2, local_len, head_dim), kv.dtype),
            pltpu.VMEM((2, chips, *row), kv.dtype),
            pltpu.VMEM((2, 2, local_len, head_dim), kv.dtype),
            pltpu.SemaphoreType.DMA,
            pltpu.SemaphoreType.DMA,
            pltpu.SemaphoreType.DMA,
            pltpu.SemaphoreType.DMA,
            pltpu.SemaphoreType.DMA((row_steps + 1,)),
            pltpu.SemaphoreType.DMA((row_steps + 1,)),
            pltpu.SemaphoreType.REGULAR((row_steps,)),
            pltpu.SemaphoreType.DMA((3,)),
            pltpu.SemaphoreType.DMA,
        ],
        compiler_params=pltpu.CompilerParams(
            collective_id=0, has_side_effects=True, vmem_limit_bytes=EXCHANGE_VMEM
        ),
        name="exchange",
    )(perm, queries, fresh, kv)


def attend_kernel(
    head_count, perm_ref, length_ref, own_ref, gathered_ref, cache_ref, out_ref,
    edge, zeros, scores, out_sem,
):
    me = lax.axis_index("wide")
    length = length_ref[perm_ref[me] // head_count]
    total_len, head_dim = gathered_ref.shape[1:]
    group_size = scores.shape[0]
    chunk = zeros.shape[0]
    chunk_count = total_len // chunk
    last = length // chunk

    def span(c):
        return pl.ds(pl.multiple_of(c * chunk, chunk), chunk)

    def each(first, stop, source):
        for kind in (0, 1):

            def one(c, carry, kind=kind):
                pltpu.make_async_copy(source(kind, c), cache_ref.at[kind, span(c)], out_sem).start()
                return carry

            lax.fori_loop(first, stop, one, 0)

    each(0, last, lambda kind, c: gathered_ref.at[kind, span(c)])
    zeros[...] = jnp.zeros_like(zeros)
    fresh = own_ref[group_size // PAIR].astype(jnp.float32)
    for kind in (0, 1):
        tile = gathered_ref[kind, span(last)].astype(jnp.float32)
        position = last * chunk + lax.broadcasted_iota(jnp.int32, tile.shape, 0)
        tile = jnp.where(position < length, tile, jnp.where(position == length, fresh[kind : kind + 1], 0.0))
        edge[kind] = tile.astype(edge.dtype)

    query = jnp.concatenate([own_ref[g].astype(jnp.float32) for g in range(group_size // PAIR)], axis=0)
    query = query.astype(own_ref.dtype)
    scale = 1.0 / math.sqrt(head_dim)

    def score(keys):
        s = lax.dot_general(query, keys, (((1,), (1,)), ((), ())), preferred_element_type=jnp.float32)
        return s * scale

    def score_full(c, top):
        s = score(gathered_ref[0, span(c)])
        scores[:, span(c)] = s
        return jnp.maximum(top, jnp.max(s, axis=1, keepdims=True))

    top = lax.fori_loop(0, last, score_full, jnp.full((group_size, 1), NEG_FILL, jnp.float32))
    visible = last * chunk + lax.broadcasted_iota(jnp.int32, (group_size, chunk), 1) <= length
    tail = jnp.where(visible, score(edge[0]), NEG_FILL)
    top = jnp.maximum(top, jnp.max(tail, axis=1, keepdims=True))
    each(last, last + 1, lambda kind, c: edge.at[kind])
    each(last + 1, chunk_count, lambda kind, c: zeros)

    def weigh(weight, values):
        high = weight.astype(jnp.bfloat16)
        low = (weight - high.astype(jnp.float32)).astype(jnp.bfloat16)
        both = jnp.concatenate([high, low], axis=0)
        return jnp.dot(both, values, preferred_element_type=jnp.float32)

    def weigh_full(c, carry):
        total, summed = carry
        weight = jnp.exp(scores[:, span(c)] - top)
        summed = summed + weigh(weight, gathered_ref[1, span(c)])
        return total + jnp.sum(weight, axis=1, keepdims=True), summed

    weight = jnp.where(visible, jnp.exp(tail - top), 0.0)
    total, summed = lax.fori_loop(
        0, last, weigh_full, (jnp.sum(weight, axis=1, keepdims=True), weigh(weight, edge[1]))
    )
    result = (summed[:group_size] + summed[group_size:]) / total
    for g in range(group_size):
        out_ref[:, g * head_dim : (g + 1) * head_dim] = result[g : g + 1].astype(out_ref.dtype)
    pltpu.make_async_copy(gathered_ref, cache_ref, out_sem).wait()


def attend(perm, lengths, own, gathered, head_count, group_size):
    kinds, total_len, head_dim = gathered.shape
    chunk = min(CHUNK, total_len)
    vmem = pl.BlockSpec(memory_space=pltpu.VMEM)
    smem = pl.BlockSpec(memory_space=pltpu.SMEM)
    any_space = pl.BlockSpec(memory_space=pl.ANY)
    return pl.pallas_call(
        functools.partial(attend_kernel, head_count),
        out_shape=(
            jax.ShapeDtypeStruct(gathered.shape, gathered.dtype),
            jax.ShapeDtypeStruct((1, group_size * head_dim), gathered.dtype),
        ),
        in_specs=[smem, smem, vmem, vmem],
        out_specs=(any_space, vmem),
        scratch_shapes=[
            pltpu.VMEM((kinds, chunk, head_dim), gathered.dtype),
            pltpu.VMEM((chunk, head_dim), gathered.dtype),
            pltpu.VMEM((group_size, total_len), jnp.float32),
            pltpu.SemaphoreType.DMA,
        ],
        compiler_params=pltpu.CompilerParams(vmem_limit_bytes=ATTEND_VMEM),
        name="attend",
    )(perm, lengths, own, gathered)


def local(kv_prefill, queries, fresh_kv, lengths, decode_slot_pair):
    devices = lax.axis_size("wide")
    kinds, seq_count, head_count, local_len, head_dim = kv_prefill.shape
    kv_rows = kv_prefill.reshape(kinds, seq_count * head_count, local_len, head_dim)
    fresh = fresh_kv.reshape(kinds, head_dim)
    gathered, own = exchange(decode_slot_pair, queries, fresh, kv_rows, devices)
    cache, attention = attend(
        decode_slot_pair, lengths, own, gathered, head_count, queries.shape[1] // head_dim
    )
    return cache[:, None], attention


def solution(mesh):
    in_specs = (
        P(None, "grp", None, "wide", None),
        P(("grp", "wide"), None),
        P(None, ("grp", "wide"), None),
        P("grp"),
        P("grp"),
    )
    out_specs = (P(None, ("grp", "wide"), None, None), P(("grp", "wide"), None))
    return jax.shard_map(local, mesh=mesh, in_specs=in_specs, out_specs=out_specs, check_vma=False)
```

```python
import functools
import math

import jax
import jax.numpy as jnp
from jax import lax
from jax.experimental import pallas as pl
from jax.experimental.pallas import tpu as pltpu
from jax.sharding import PartitionSpec as P

MESH = pl.DeviceIdType.MESH
NEG_FILL = -1e30
PAIR = 2
CHUNK = 512
WIDE = 2048
EARLY = 5
EXCHANGE_VMEM = 58 << 20
ATTEND_VMEM = 12 << 20


def exchange_kernel(
    devices,
    perm_source,
    query_ref,
    fresh_ref,
    kv_ref,
    gathered_ref,
    own_ref,
    stage,
    ordered,
    rows,
    passing,
    stage_sem,
    local_sem,
    send_sem,
    recv_sem,
    row_send,
    row_recv,
    near_sem,
    pass_send,
    pass_recv,
    query_row,
    fresh_rows,
    small_sem,
    perm_ref,
):
    chips = devices // 2
    half = chips // 2
    me = lax.axis_index("wide")
    chip = me // 2
    core = lax.rem(me, 2)
    partner = chip * 2 + 1 - core
    local_len = kv_ref.shape[2]

    def device(offset, which):
        return lax.rem(chip + offset + chips, chips) * 2 + which

    def remote(src, dst, send, recv, target):
        return pltpu.make_async_remote_copy(
            src_ref=src,
            dst_ref=dst,
            send_sem=send,
            recv_sem=recv,
            device_id={"wide": target},
            device_id_type=MESH,
        )

    def signal(sem, target):
        pl.semaphore_signal(sem, inc=1, device_id={"wide": target}, device_id_type=MESH)

    barrier = pltpu.get_barrier_semaphore()
    signal(barrier, partner)
    for offset in (1, -1):
        for which in (0, 1):
            signal(barrier, device(offset, which))
    fill = pltpu.make_async_copy(kv_ref, stage, stage_sem)
    slots_in = pltpu.make_async_copy(perm_source, perm_ref, small_sem.at[2])
    slots_in.start()
    fill.start()
    bring = [
        pltpu.make_async_copy(query_ref, query_row, small_sem.at[0]),
        pltpu.make_async_copy(fresh_ref, fresh_rows, small_sem.at[1]),
    ]
    for copy in bring:
        copy.start()
    slots_in.wait()
    fill.wait()

    def place(slot):
        ordered[slot] = stage[:, perm_ref[slot]]

    def place_span(first, last):
        def one(k, carry):
            place(lax.rem(chip * 2 + (devices + first) + k, devices))
            return carry

        lax.fori_loop(0, last - first, one, 0)

    place_span(-4, 6)
    pl.semaphore_wait(barrier, 5)

    final = gathered_ref.at[:, pl.ds(me * local_len, local_len)]
    keep = pltpu.make_async_copy(ordered.at[me], final, local_sem)
    keep.start()

    def send_block(target):
        remote(ordered.at[target], final, send_sem, recv_sem, target).start()

    def send_both(distance, cores=(0, 1)):
        for which in cores:
            for sign in (1, -1):
                send_block(device(sign * distance, which))

    def widen(level):
        reach = 1 << level
        for sign in (1, -1):
            signal(near_sem.at[level], device(sign * reach, core))
        pl.semaphore_wait(near_sem.at[level], 2)

    send_block(partner)
    send_both(1, (1,))
    place_span(6, devices - 4)
    for copy in bring:
        copy.wait()
    head_dim = kv_ref.shape[3]
    group_size = query_ref.shape[1] // head_dim
    query = query_row[...].astype(jnp.float32)
    for g in range(0, group_size, PAIR):
        heads = [query[:, h * head_dim : (h + 1) * head_dim] for h in range(g, g + PAIR)]
        rows[0, 0, g // PAIR] = jnp.concatenate(heads, axis=0).astype(jnp.bfloat16)
    rows[0, 0, group_size // PAIR] = fresh_rows[...]
    sent_to = 1
    level = 0
    while (1 << level) < half:
        widen(level)
        level += 1
        if level < half.bit_length() - 1:
            for distance in range(sent_to + 1, min((1 << level), EARLY) + 1):
                send_both(distance, (distance % 2,))
                sent_to = distance

    turn = 1 - 2 * core

    def row_copy(step):
        size = 1 << step
        return remote(
            rows.at[0, pl.ds(0, size)],
            rows.at[0, pl.ds(size, size)],
            row_send.at[step],
            row_recv.at[step],
            device(turn * (chips >> (step + 1)), core),
        )

    side = jnp.where(chip >= half, 1, -1)

    def turns(c):
        quarter = chips // 4
        return ((c >= chips - quarter) & (lax.rem(c, 2) == 0)) | ((c < quarter) & (lax.rem(c, 2) == 1))

    turned = turns(chip)
    relaying = turns(lax.rem(chip + side + chips, chips))

    def detour():
        both = ordered.at[pl.ds(device(half, 0), 2)]
        return remote(both, passing, pass_send.at[0], pass_recv, device(-side, core))

    def forward(which):
        origin = device(side, core)
        return remote(
            passing.at[which],
            gathered_ref.at[:, pl.ds(origin * local_len, local_len)],
            pass_send.at[1 + which],
            recv_sem,
            device(half + side, which),
        )

    @pl.when(turned)
    def _():
        detour().start()

    @pl.when(jnp.logical_not(turned))
    def _():
        send_block(device(half, 0))
        send_block(device(half, 1))

    row_steps = chips.bit_length() - 1
    row_copy(0).start()
    step = 0
    rounds = [(distance, (0, 1)) for distance in range(half - 1, sent_to, -1)]
    rounds += [(distance, (1 - distance % 2,)) for distance in range(sent_to, 0, -1)]
    for number, (distance, cores) in enumerate(rounds):
        send_both(distance, cores)
        if number == 2:

            @pl.when(relaying)
            def _():
                detour().wait_recv()
                forward(0).start()
                forward(1).start()

        if number % 2 == 1:
            if step < row_steps:
                row_copy(step).wait()
                step += 1
                if step < row_steps:
                    row_copy(step).start()
    while step < row_steps:
        row_copy(step).wait()
        step += 1
        if step < row_steps:
            row_copy(step).start()
    across = remote(rows.at[0], rows.at[1], row_send.at[row_steps], row_recv.at[row_steps], partner)
    across.start()
    across.wait()

    item = perm_ref[me]
    item_core = lax.rem(item, 2)
    same = 1 - lax.rem(item_core + core, 2)
    offset = lax.rem((1 - 2 * item_core) * (chip - item // 2) + chips, chips)
    place_of = 0
    for bit in range(row_steps):
        place_of += lax.rem(offset // (1 << bit), 2) * (chips >> (bit + 1))
    own_ref[...] = rows[1 - same, place_of]

    keep.wait()
    def blocks(count):
        many = ordered.at[pl.ds(0, count)]
        return remote(many, many, send_sem, recv_sem, partner)

    @pl.when(turned)
    def _():
        detour().wait_send()
        blocks(devices - 3).wait_send()

    @pl.when(jnp.logical_not(turned))
    def _():
        blocks(devices - 1).wait_send()

    @pl.when(relaying)
    def _():
        forward(0).wait_send()
        forward(1).wait_send()

    blocks(devices - 1).wait_recv()


def exchange(perm, queries, fresh, kv, devices):
    items, local_len, head_dim = kv.shape[1:]
    chips = devices // 2
    row_steps = chips.bit_length() - 1
    any_space = pl.BlockSpec(memory_space=pl.ANY)
    vmem = pl.BlockSpec(memory_space=pltpu.VMEM)
    row = (queries.shape[1] // head_dim // PAIR + 1, PAIR, head_dim)
    return pl.pallas_call(
        functools.partial(exchange_kernel, devices),
        out_shape=(
            pltpu.VMEM((2, devices * local_len, head_dim), kv.dtype),
            pltpu.VMEM(row, kv.dtype),
        ),
        in_specs=[any_space] * 4,
        out_specs=(vmem, vmem),
        scratch_shapes=[
            pltpu.VMEM((2, items, local_len, head_dim), kv.dtype),
            pltpu.VMEM((items, 2, local_len, head_dim), kv.dtype),
            pltpu.VMEM((2, chips, *row), kv.dtype),
            pltpu.VMEM((2, 2, local_len, head_dim), kv.dtype),
            pltpu.SemaphoreType.DMA,
            pltpu.SemaphoreType.DMA,
            pltpu.SemaphoreType.DMA,
            pltpu.SemaphoreType.DMA,
            pltpu.SemaphoreType.DMA((row_steps + 1,)),
            pltpu.SemaphoreType.DMA((row_steps + 1,)),
            pltpu.SemaphoreType.REGULAR((row_steps,)),
            pltpu.SemaphoreType.DMA((3,)),
            pltpu.SemaphoreType.DMA,
            pltpu.VMEM(queries.shape, kv.dtype),
            pltpu.VMEM(fresh.shape, kv.dtype),
            pltpu.SemaphoreType.DMA((3,)),
            pltpu.SMEM(perm.shape, perm.dtype),
        ],
        compiler_params=pltpu.CompilerParams(
            collective_id=0, has_side_effects=True, vmem_limit_bytes=EXCHANGE_VMEM
        ),
        name="exchange",
    )(perm, queries, fresh, kv)


def attend_kernel(
    head_count, perm_ref, length_ref, own_ref, gathered_ref, cache_ref, out_ref,
    edge, zeros, scores, out_sem,
):
    me = lax.axis_index("wide")
    length = length_ref[perm_ref[me] // head_count]
    total_len, head_dim = gathered_ref.shape[1:]
    group_size = scores.shape[0]
    chunk = zeros.shape[0]
    chunk_count = total_len // chunk
    last = length // chunk

    def span(c):
        return pl.ds(pl.multiple_of(c * chunk, chunk), chunk)

    def each(first, stop, source):
        for kind in (0, 1):

            def one(c, carry, kind=kind):
                pltpu.make_async_copy(source(kind, c), cache_ref.at[kind, span(c)], out_sem).start()
                return carry

            lax.fori_loop(first, stop, one, 0)

    each(0, last, lambda kind, c: gathered_ref.at[kind, span(c)])
    zeros[...] = jnp.zeros_like(zeros)
    fresh = own_ref[group_size // PAIR].astype(jnp.float32)
    for kind in (0, 1):
        tile = gathered_ref[kind, span(last)].astype(jnp.float32)
        position = last * chunk + lax.broadcasted_iota(jnp.int32, tile.shape, 0)
        tile = jnp.where(position < length, tile, jnp.where(position == length, fresh[kind : kind + 1], 0.0))
        edge[kind] = tile.astype(edge.dtype)

    heads = jnp.concatenate([own_ref[g].astype(jnp.float32) for g in range(group_size // PAIR)], axis=0)
    query = heads.astype(own_ref.dtype)
    scale = 1.0 / math.sqrt(head_dim)
    wide = min(WIDE, total_len)
    turns = (length + wide - 1) // wide
    newest = jnp.sum(heads * fresh[0:1], axis=1, keepdims=True) * scale

    def wide_span(c):
        return pl.ds(pl.multiple_of(c * wide, wide), wide)

    def score(c, top):
        keys = gathered_ref[0, wide_span(c)]
        s = lax.dot_general(query, keys, (((1,), (1,)), ((), ())), preferred_element_type=jnp.float32)
        position = c * wide + lax.broadcasted_iota(jnp.int32, s.shape, 1)
        s = jnp.where(position < length, s * scale, NEG_FILL)
        scores[:, wide_span(c)] = s
        return jnp.maximum(top, jnp.max(s, axis=1, keepdims=True))

    top = lax.fori_loop(0, turns, score, newest)
    each(last, last + 1, lambda kind, c: edge.at[kind])
    each(last + 1, chunk_count, lambda kind, c: zeros)

    def weigh(c, carry):
        total, summed = carry
        weight = jnp.exp(scores[:, wide_span(c)] - top)
        high = weight.astype(jnp.bfloat16)
        low = (weight - high.astype(jnp.float32)).astype(jnp.bfloat16)
        both = jnp.concatenate([high, low], axis=0)
        values = gathered_ref[1, wide_span(c)]
        summed = summed + jnp.dot(both, values, preferred_element_type=jnp.float32)
        return total + jnp.sum(weight, axis=1, keepdims=True), summed

    weight = jnp.exp(newest - top)
    total, summed = lax.fori_loop(
        0, turns, weigh, (weight, jnp.zeros((2 * group_size, head_dim), jnp.float32))
    )
    result = (summed[:group_size] + summed[group_size:] + weight * fresh[1:2]) / total
    for g in range(group_size):
        out_ref[:, g * head_dim : (g + 1) * head_dim] = result[g : g + 1].astype(out_ref.dtype)
    pltpu.make_async_copy(gathered_ref, cache_ref, out_sem).wait()


def attend(perm, lengths, own, gathered, head_count, group_size):
    kinds, total_len, head_dim = gathered.shape
    chunk = min(CHUNK, total_len)
    vmem = pl.BlockSpec(memory_space=pltpu.VMEM)
    smem = pl.BlockSpec(memory_space=pltpu.SMEM)
    any_space = pl.BlockSpec(memory_space=pl.ANY)
    return pl.pallas_call(
        functools.partial(attend_kernel, head_count),
        out_shape=(
            jax.ShapeDtypeStruct(gathered.shape, gathered.dtype),
            jax.ShapeDtypeStruct((1, group_size * head_dim), gathered.dtype),
        ),
        in_specs=[smem, smem, vmem, vmem],
        out_specs=(any_space, vmem),
        scratch_shapes=[
            pltpu.VMEM((kinds, chunk, head_dim), gathered.dtype),
            pltpu.VMEM((chunk, head_dim), gathered.dtype),
            pltpu.VMEM((group_size, total_len), jnp.float32),
            pltpu.SemaphoreType.DMA,
        ],
        compiler_params=pltpu.CompilerParams(vmem_limit_bytes=ATTEND_VMEM),
        name="attend",
    )(perm, lengths, own, gathered)


def local(kv_prefill, queries, fresh_kv, lengths, decode_slot_pair):
    devices = lax.axis_size("wide")
    kinds, seq_count, head_count, local_len, head_dim = kv_prefill.shape
    kv_rows = kv_prefill.reshape(kinds, seq_count * head_count, local_len, head_dim)
    fresh = fresh_kv.reshape(kinds, head_dim)
    gathered, own = exchange(decode_slot_pair, queries, fresh, kv_rows, devices)
    cache, attention = attend(
        decode_slot_pair, lengths, own, gathered, head_count, queries.shape[1] // head_dim
    )
    return cache[:, None], attention


def solution(mesh):
    in_specs = (
        P(None, "grp", None, "wide", None),
        P(("grp", "wide"), None),
        P(None, ("grp", "wide"), None),
        P("grp"),
        P("grp"),
    )
    out_specs = (P(None, ("grp", "wide"), None, None), P(("grp", "wide"), None))
    return jax.shard_map(local, mesh=mesh, in_specs=in_specs, out_specs=out_specs, check_vma=False)
```

```python
import functools
import math

import jax
import jax.numpy as jnp
from jax import lax
from jax.experimental import pallas as pl
from jax.experimental.pallas import tpu as pltpu
from jax.sharding import PartitionSpec as P

MESH = pl.DeviceIdType.MESH
NEG_FILL = -1e30
PAIR = 2
CHUNK = 512
WIDE = 2048
EARLY = 5
EXCHANGE_VMEM = 58 << 20
ATTEND_VMEM = 12 << 20


def exchange_kernel(
    devices,
    perm_source,
    query_ref,
    fresh_ref,
    kv_ref,
    gathered_ref,
    own_ref,
    stage,
    ordered,
    rows,
    passing,
    stage_sem,
    local_sem,
    send_sem,
    recv_sem,
    row_send,
    row_recv,
    near_sem,
    pass_send,
    pass_recv,
    query_row,
    fresh_rows,
    small_sem,
    perm_ref,
):
    chips = devices // 2
    half = chips // 2
    me = lax.axis_index("wide")
    chip = me // 2
    core = lax.rem(me, 2)
    partner = chip * 2 + 1 - core
    local_len = kv_ref.shape[2]

    def device(offset, which):
        return lax.rem(chip + offset + chips, chips) * 2 + which

    def remote(src, dst, send, recv, target):
        return pltpu.make_async_remote_copy(
            src_ref=src,
            dst_ref=dst,
            send_sem=send,
            recv_sem=recv,
            device_id={"wide": target},
            device_id_type=MESH,
        )

    def signal(sem, target):
        pl.semaphore_signal(sem, inc=1, device_id={"wide": target}, device_id_type=MESH)

    barrier = pltpu.get_barrier_semaphore()
    signal(barrier, partner)
    for offset in (1, -1):
        for which in (0, 1):
            signal(barrier, device(offset, which))
    fill = pltpu.make_async_copy(kv_ref, stage, stage_sem)
    slots_in = pltpu.make_async_copy(perm_source, perm_ref, small_sem.at[2])
    slots_in.start()
    fill.start()
    bring = [
        pltpu.make_async_copy(query_ref, query_row, small_sem.at[0]),
        pltpu.make_async_copy(fresh_ref, fresh_rows, small_sem.at[1]),
    ]
    for copy in bring:
        copy.start()
    slots_in.wait()
    fill.wait()

    def place(slot):
        ordered[slot] = stage[:, perm_ref[slot]]

    def place_span(first, last):
        def one(k, carry):
            place(lax.rem(chip * 2 + (devices + first) + k, devices))
            return carry

        lax.fori_loop(0, last - first, one, 0)

    place_span(-4, 6)
    pl.semaphore_wait(barrier, 5)

    final = gathered_ref.at[:, pl.ds(me * local_len, local_len)]
    keep = pltpu.make_async_copy(ordered.at[me], final, local_sem)
    keep.start()

    def send_block(target):
        remote(ordered.at[target], final, send_sem, recv_sem, target).start()

    def send_both(distance, cores=(0, 1)):
        for which in cores:
            for sign in (1, -1):
                send_block(device(sign * distance, which))

    def widen(level):
        reach = 1 << level
        for sign in (1, -1):
            signal(near_sem.at[level], device(sign * reach, core))
        pl.semaphore_wait(near_sem.at[level], 2)

    send_block(partner)
    send_both(1, (1,))
    place_span(6, devices - 4)
    for copy in bring:
        copy.wait()
    head_dim = kv_ref.shape[3]
    group_size = query_ref.shape[1] // head_dim
    query = query_row[...].astype(jnp.float32)
    for g in range(0, group_size, PAIR):
        heads = [query[:, h * head_dim : (h + 1) * head_dim] for h in range(g, g + PAIR)]
        rows[0, 0, g // PAIR] = jnp.concatenate(heads, axis=0).astype(jnp.bfloat16)
    rows[0, 0, group_size // PAIR] = fresh_rows[...]
    sent_to = 1
    level = 0
    while (1 << level) < half:
        widen(level)
        level += 1
        if level < half.bit_length() - 1:
            for distance in range(sent_to + 1, min((1 << level), EARLY) + 1):
                send_both(distance, (distance % 2,))
                sent_to = distance

    turn = 1 - 2 * core

    def row_copy(step):
        size = 1 << step
        return remote(
            rows.at[0, pl.ds(0, size)],
            rows.at[0, pl.ds(size, size)],
            row_send.at[step],
            row_recv.at[step],
            device(turn * (chips >> (step + 1)), core),
        )

    side = jnp.where(chip >= half, 1, -1)

    def turns(c):
        quarter = chips // 4
        return ((c >= chips - quarter) & (lax.rem(c, 2) == 0)) | ((c < quarter) & (lax.rem(c, 2) == 1))

    turned = turns(chip)
    relaying = turns(lax.rem(chip + side + chips, chips))

    def detour():
        both = ordered.at[pl.ds(device(half, 0), 2)]
        return remote(both, passing, pass_send.at[0], pass_recv, device(-side, core))

    def forward(which):
        origin = device(side, core)
        return remote(
            passing.at[which],
            gathered_ref.at[:, pl.ds(origin * local_len, local_len)],
            pass_send.at[1 + which],
            recv_sem,
            device(half + side, which),
        )

    @pl.when(turned)
    def _():
        detour().start()

    @pl.when(jnp.logical_not(turned))
    def _():
        send_block(device(half, 0))
        send_block(device(half, 1))

    row_steps = chips.bit_length() - 1
    row_copy(0).start()
    step = 0
    rounds = [(distance, (0, 1)) for distance in range(half - 1, sent_to, -1)]
    rounds += [(distance, (1 - distance % 2,)) for distance in range(sent_to, 0, -1)]
    for number, (distance, cores) in enumerate(rounds):
        send_both(distance, cores)
        if number == 2:

            @pl.when(relaying)
            def _():
                detour().wait_recv()
                forward(0).start()
                forward(1).start()

        if number % 2 == 1:
            if step < row_steps:
                row_copy(step).wait()
                step += 1
                if step < row_steps:
                    row_copy(step).start()
    while step < row_steps:
        row_copy(step).wait()
        step += 1
        if step < row_steps:
            row_copy(step).start()
    across = remote(rows.at[0], rows.at[1], row_send.at[row_steps], row_recv.at[row_steps], partner)
    across.start()
    across.wait()

    item = perm_ref[me]
    item_core = lax.rem(item, 2)
    same = 1 - lax.rem(item_core + core, 2)
    offset = lax.rem((1 - 2 * item_core) * (chip - item // 2) + chips, chips)
    place_of = 0
    for bit in range(row_steps):
        place_of += lax.rem(offset // (1 << bit), 2) * (chips >> (bit + 1))
    own_ref[...] = rows[1 - same, place_of]

    keep.wait()
    def blocks(count):
        many = ordered.at[pl.ds(0, count)]
        return remote(many, many, send_sem, recv_sem, partner)

    @pl.when(turned)
    def _():
        detour().wait_send()
        blocks(devices - 3).wait_send()

    @pl.when(jnp.logical_not(turned))
    def _():
        blocks(devices - 1).wait_send()

    @pl.when(relaying)
    def _():
        forward(0).wait_send()
        forward(1).wait_send()

    blocks(devices - 1).wait_recv()


def exchange(perm, queries, fresh, kv, devices):
    items, local_len, head_dim = kv.shape[1:]
    chips = devices // 2
    row_steps = chips.bit_length() - 1
    any_space = pl.BlockSpec(memory_space=pl.ANY)
    vmem = pl.BlockSpec(memory_space=pltpu.VMEM)
    row = (queries.shape[1] // head_dim // PAIR + 1, PAIR, head_dim)
    return pl.pallas_call(
        functools.partial(exchange_kernel, devices),
        out_shape=(
            pltpu.VMEM((2, devices * local_len, head_dim), kv.dtype),
            pltpu.VMEM(row, kv.dtype),
        ),
        in_specs=[any_space] * 4,
        out_specs=(vmem, vmem),
        scratch_shapes=[
            pltpu.VMEM((2, items, local_len, head_dim), kv.dtype),
            pltpu.VMEM((items, 2, local_len, head_dim), kv.dtype),
            pltpu.VMEM((2, chips, *row), kv.dtype),
            pltpu.VMEM((2, 2, local_len, head_dim), kv.dtype),
            pltpu.SemaphoreType.DMA,
            pltpu.SemaphoreType.DMA,
            pltpu.SemaphoreType.DMA,
            pltpu.SemaphoreType.DMA,
            pltpu.SemaphoreType.DMA((row_steps + 1,)),
            pltpu.SemaphoreType.DMA((row_steps + 1,)),
            pltpu.SemaphoreType.REGULAR((row_steps,)),
            pltpu.SemaphoreType.DMA((3,)),
            pltpu.SemaphoreType.DMA,
            pltpu.VMEM(queries.shape, kv.dtype),
            pltpu.VMEM(fresh.shape, kv.dtype),
            pltpu.SemaphoreType.DMA((3,)),
            pltpu.SMEM(perm.shape, perm.dtype),
        ],
        compiler_params=pltpu.CompilerParams(
            collective_id=0, has_side_effects=True, vmem_limit_bytes=EXCHANGE_VMEM
        ),
        name="exchange",
    )(perm, queries, fresh, kv)


def attend_kernel(
    head_count, perm_ref, length_ref, own_ref, gathered_ref, cache_ref, out_ref,
    edge, zeros, scores, out_row, out_sem, row_sem,
):
    me = lax.axis_index("wide")
    length = length_ref[perm_ref[me] // head_count]
    total_len, head_dim = gathered_ref.shape[1:]
    group_size = scores.shape[0]
    chunk = zeros.shape[0]
    chunk_count = total_len // chunk
    last = length // chunk

    def span(c):
        return pl.ds(pl.multiple_of(c * chunk, chunk), chunk)

    def each(first, stop, source):
        for kind in (0, 1):

            def one(c, carry, kind=kind):
                pltpu.make_async_copy(source(kind, c), cache_ref.at[kind, span(c)], out_sem).start()
                return carry

            lax.fori_loop(first, stop, one, 0)

    each(0, last, lambda kind, c: gathered_ref.at[kind, span(c)])
    zeros[...] = jnp.zeros_like(zeros)
    fresh = own_ref[group_size // PAIR].astype(jnp.float32)
    for kind in (0, 1):
        tile = gathered_ref[kind, span(last)].astype(jnp.float32)
        position = last * chunk + lax.broadcasted_iota(jnp.int32, tile.shape, 0)
        tile = jnp.where(position < length, tile, jnp.where(position == length, fresh[kind : kind + 1], 0.0))
        edge[kind] = tile.astype(edge.dtype)

    heads = jnp.concatenate([own_ref[g].astype(jnp.float32) for g in range(group_size // PAIR)], axis=0)
    query = heads.astype(own_ref.dtype)
    scale = 1.0 / math.sqrt(head_dim)
    wide = min(WIDE, total_len)
    turns = (length + wide - 1) // wide
    newest = jnp.sum(heads * fresh[0:1], axis=1, keepdims=True) * scale

    def wide_span(c):
        return pl.ds(pl.multiple_of(c * wide, wide), wide)

    def score(c, top):
        keys = gathered_ref[0, wide_span(c)]
        s = lax.dot_general(query, keys, (((1,), (1,)), ((), ())), preferred_element_type=jnp.float32)
        position = c * wide + lax.broadcasted_iota(jnp.int32, s.shape, 1)
        s = jnp.where(position < length, s * scale, NEG_FILL)
        scores[:, wide_span(c)] = s
        return jnp.maximum(top, jnp.max(s, axis=1, keepdims=True))

    top = lax.fori_loop(0, turns, score, newest)
    each(last, last + 1, lambda kind, c: edge.at[kind])
    each(last + 1, chunk_count, lambda kind, c: zeros)

    def weigh(c, carry):
        total, summed = carry
        weight = jnp.exp(scores[:, wide_span(c)] - top)
        high = weight.astype(jnp.bfloat16)
        low = (weight - high.astype(jnp.float32)).astype(jnp.bfloat16)
        both = jnp.concatenate([high, low], axis=0)
        values = gathered_ref[1, wide_span(c)]
        summed = summed + jnp.dot(both, values, preferred_element_type=jnp.float32)
        return total + jnp.sum(weight, axis=1, keepdims=True), summed

    weight = jnp.exp(newest - top)
    total, summed = lax.fori_loop(
        0, turns, weigh, (weight, jnp.zeros((2 * group_size, head_dim), jnp.float32))
    )
    result = (summed[:group_size] + summed[group_size:] + weight * fresh[1:2]) / total
    for g in range(group_size):
        out_row[:, g * head_dim : (g + 1) * head_dim] = result[g : g + 1].astype(out_row.dtype)
    deliver = pltpu.make_async_copy(out_row, out_ref, row_sem)
    deliver.start()
    pltpu.make_async_copy(gathered_ref, cache_ref, out_sem).wait()
    deliver.wait()


def attend(perm, lengths, own, gathered, head_count, group_size):
    kinds, total_len, head_dim = gathered.shape
    chunk = min(CHUNK, total_len)
    vmem = pl.BlockSpec(memory_space=pltpu.VMEM)
    smem = pl.BlockSpec(memory_space=pltpu.SMEM)
    any_space = pl.BlockSpec(memory_space=pl.ANY)
    return pl.pallas_call(
        functools.partial(attend_kernel, head_count),
        out_shape=(
            jax.ShapeDtypeStruct(gathered.shape, gathered.dtype),
            jax.ShapeDtypeStruct((1, group_size * head_dim), gathered.dtype),
        ),
        in_specs=[smem, smem, vmem, vmem],
        out_specs=(any_space, any_space),
        scratch_shapes=[
            pltpu.VMEM((kinds, chunk, head_dim), gathered.dtype),
            pltpu.VMEM((chunk, head_dim), gathered.dtype),
            pltpu.VMEM((group_size, total_len), jnp.float32),
            pltpu.VMEM((1, group_size * head_dim), gathered.dtype),
            pltpu.SemaphoreType.DMA,
            pltpu.SemaphoreType.DMA,
        ],
        compiler_params=pltpu.CompilerParams(vmem_limit_bytes=ATTEND_VMEM),
        name="attend",
    )(perm, lengths, own, gathered)


def local(kv_prefill, queries, fresh_kv, lengths, decode_slot_pair):
    devices = lax.axis_size("wide")
    kinds, seq_count, head_count, local_len, head_dim = kv_prefill.shape
    kv_rows = kv_prefill.reshape(kinds, seq_count * head_count, local_len, head_dim)
    fresh = fresh_kv.reshape(kinds, head_dim)
    gathered, own = exchange(decode_slot_pair, queries, fresh, kv_rows, devices)
    cache, attention = attend(
        decode_slot_pair, lengths, own, gathered, head_count, queries.shape[1] // head_dim
    )
    return cache[:, None], attention


def solution(mesh):
    in_specs = (
        P(None, "grp", None, "wide", None),
        P(("grp", "wide"), None),
        P(None, ("grp", "wide"), None),
        P("grp"),
        P("grp"),
    )
    out_specs = (P(None, ("grp", "wide"), None, None), P(("grp", "wide"), None))
    return jax.shard_map(local, mesh=mesh, in_specs=in_specs, out_specs=out_specs, check_vma=False)
```
